32 devices in a mesh: member: 4 (over x, core), region: 8 (over z, y).
Axes of the slice: x: 2, y: 2, z: 4, core: 2. Of those that a mesh axis runs over, the one named last changes fastest.
Arguments:
- background: bfloat16 [4, 8, 96, 256, 64], P(None, 'region', None, 'member'), may hold values from -6 to 6
- obs_ensemble: bfloat16 [4, 8, 1, 256, 1024], P(None, 'region', None, 'member'), may hold values from -6 to 6
- obs_value: float32 [4, 8, 1, 1024], P('member', 'region'), may hold values from -12 to 12
- obs_weight: float32 [4, 8, 1, 1024], P('member', 'region'), may hold values from 0.05 to 1
- stencil: int32 [4, 8, 4, 64], P('member', 'region'), may hold values from 0 to 31, as said below
- stencil_weight: float32 [4, 8, 4, 64], P('member', 'region'), may hold values from 0.05 to 1
- block_target: int32 [4, 8, 8], replicated, may hold values from 0 to 255, as said below
Outputs:
- analysis: float32 [8, 96, 256, 256], P('region', None, 'member')
The draws below stay inside these ranges and needn't reach their ends.
Inputs may be any that keep to these rules, and one draw needn't show every extreme that they name: `stencil`: each entry names a coarse point whose band and patch each differ by at most one from those of its column. `block_target`: A permutation of all blocks. The 8 blocks of one band in one patch go to distinct owners (owner = value // 32); the blocks of one patch go to any owner at most 4 at a time, and exactly 4 to some owner.
All inputs are finite; a program needn't handle non-finite values.
Results may differ from the reference program's by a relative error of at most 0.0003.
Values may be sent and summed in bfloat16 or wider, within the bound.
No kernel may reach another device: no remote copies, remote signals or barrier semaphores. Data moves between devices by JAX's collectives and lax.ppermute only.
A program may use at most 128 MiB of HBM per device.

```python
import math
import jax
import jax.numpy as jnp
from jax import lax

K = 256
V = 96
OBS = 1024
POINTS_PER_PATCH = 1
COL_DEV = 64
BLK_DEV = 8
SWEEPS = 8
BANDS = 4
PATCHES = 8


def band_offsets(band_key):
    first_key, second_key = jax.random.split(band_key)
    others = jax.random.permutation(first_key, PATCHES - 1)[:BLK_DEV - 1].astype(jnp.int32) + 1
    chosen = jnp.concatenate([jnp.zeros((1,), jnp.int32), others])
    return jax.random.permutation(second_key, chosen)


def owner_order(owner_key):
    return jax.random.permutation(owner_key, BANDS * BLK_DEV).astype(jnp.int32)


def draw_block_target(key, part):
    subkeys = jax.random.split(jax.random.fold_in(key, 41), 3)
    offsets = jax.vmap(band_offsets)(jax.random.split(subkeys[0], BANDS))
    relabel = jax.random.permutation(subkeys[1], PATCHES).astype(jnp.int32)
    patch_ids = jnp.arange(PATCHES, dtype=jnp.int32)
    owners = relabel[(patch_ids[None, :, None] + offsets[:, None, :]) % PATCHES]
    flat_owner = owners.reshape(-1)
    owner_hot = (flat_owner[:, None] == patch_ids[None, :]).astype(jnp.int32)
    ranked = jnp.sum((jnp.cumsum(owner_hot, axis=0) - 1) * owner_hot, axis=1)
    per_owner = BANDS * BLK_DEV
    orders = jax.vmap(owner_order)(jax.random.split(subkeys[2], PATCHES))
    places = orders[flat_owner, ranked]
    return (flat_owner * per_owner + places).reshape(BANDS, PATCHES, BLK_DEV).astype(jnp.int32)


def draw_stencil(key, part):
    subkeys = jax.random.split(jax.random.fold_in(key, 53), 3)
    stencil_shape = (BANDS, PATCHES, 4, COL_DEV)
    band_step = jax.random.randint(subkeys[0], stencil_shape, -1, 2)
    patch_step = jax.random.randint(subkeys[1], stencil_shape, -1, 2)
    near_band = jnp.clip(jnp.arange(BANDS, dtype=jnp.int32)[:, None, None, None] + band_step, 0, BANDS - 1)
    near_patch = jnp.clip(jnp.arange(PATCHES, dtype=jnp.int32)[None, :, None, None] + patch_step, 0, PATCHES - 1)
    within = jax.random.randint(subkeys[2], stencil_shape, 0, POINTS_PER_PATCH)
    return ((near_band * PATCHES + near_patch) * POINTS_PER_PATCH + within).astype(jnp.int32)


def shard_levels(key, extent, pieces, smallest, high):
    level, own = 1.0, jax.random.fold_in(key, 6)
    for axis_at, blocks in pieces:
        draws = jnp.exp(jax.random.uniform(jax.random.fold_in(own, axis_at), (blocks,), jnp.float32, smallest / len(pieces), high / len(pieces)))
        level = level * jnp.repeat(draws, extent[axis_at] // blocks).reshape([-1 if axis == axis_at else 1 for axis in range(len(extent))])
    return level


def centred(key, shape, scale, reach, cuts=(), held_as=jnp.bfloat16):
    result = scale * jax.random.normal(key, shape, jnp.float32)
    if cuts:
        result = result * shard_levels(key, shape, cuts, -0.22, 0.18)
    return jnp.clip(result, -reach, reach).astype(held_as)


def setup_inputs(seed: int = 0) -> dict:
    splits = jax.random.split(jax.random.key(seed), 8)
    background = centred(splits[0], (BANDS, PATCHES, V, K, COL_DEV), 1.0, 6.0, ((1, 8), (3, 4)))
    obs_ensemble = centred(splits[1], (BANDS, PATCHES, POINTS_PER_PATCH, K, OBS), 1.0, 6.0, ((1, 8), (3, 4)))
    obs_value = centred(splits[2], (BANDS, PATCHES, POINTS_PER_PATCH, OBS), 2.0, 12.0, ((0, 4), (1, 8)), jnp.float32)
    obs_weight = jnp.clip(jnp.exp(math.log(1.0) - 2.9957323 * jax.random.uniform(splits[3], (BANDS, PATCHES, POINTS_PER_PATCH, OBS), jnp.float32) ** shard_levels(splits[3], (BANDS, PATCHES, POINTS_PER_PATCH, OBS), ((0, 4), (1, 8)), -0.2, 0.2)), 0.05, 1.0)
    stencil = draw_stencil(jax.random.fold_in(splits[7], 71), 0)
    stencil_weight = jnp.clip(jnp.exp(math.log(1.0) - 2.9957323 * jax.random.uniform(splits[5], (BANDS, PATCHES, 4, COL_DEV), jnp.float32) ** shard_levels(splits[5], (BANDS, PATCHES, 4, COL_DEV), ((0, 4), (1, 8)), -0.2, 0.2)), 0.05, 1.0)
    block_target = draw_block_target(jax.random.fold_in(splits[7], 71), 0)
    return dict(background=background, obs_ensemble=obs_ensemble, obs_value=obs_value, obs_weight=obs_weight, stencil=stencil, stencil_weight=stencil_weight, block_target=block_target)


largest_value = lax.Precision.HIGHEST

def build_transforms(obs_pert, departure, obs_weight):
    scaled = obs_pert * obs_weight[:, None, :]
    gram_matrix = jnp.einsum('nko,nlo->nkl', scaled, obs_pert, precision=largest_value)
    forcing = jnp.einsum('nko,no->nk', scaled, departure, precision=largest_value)
    members = gram_matrix.shape[-1]
    identity = jnp.eye(members, dtype=jnp.float32)
    system = gram_matrix + (members - 1.0) * identity
    norm_sum = jnp.sqrt(lax.optimization_barrier(jnp.sum(system * system, axis=(1, 2))))
    iterate = system / norm_sum[:, None, None]
    inverse = jnp.broadcast_to(identity, system.shape)
    for repeat_step in range(SWEEPS):
        factor = 1.5 * identity - 0.5 * jnp.matmul(inverse, iterate, precision=largest_value)
        iterate = jnp.matmul(iterate, factor, precision=largest_value)
        inverse = jnp.matmul(factor, inverse, precision=largest_value)
    first_pass = jnp.einsum('nkl,nl->nk', inverse, forcing, precision=largest_value)
    mean_weight = jnp.einsum('nkl,nl->nk', inverse, first_pass, precision=largest_value) / norm_sum[:, None]
    spread = jnp.sqrt((members - 1.0) / norm_sum)[:, None, None] * inverse
    return spread + mean_weight[:, :, None]

def reference(background, obs_ensemble, obs_value, obs_weight, stencil, stencil_weight, block_target):
    band_count, patch_list, levels, members, columns = background.shape
    points = obs_ensemble.shape[2]
    states = background.astype(jnp.float32)
    state_mean = lax.optimization_barrier(jnp.mean(states, axis=3))
    state_pert = states - state_mean[:, :, :, None, :]
    ensemble = obs_ensemble.reshape(band_count * patch_list, points, members, -1)
    values = obs_value.reshape(band_count * patch_list, points, -1)
    weights = obs_weight.reshape(band_count * patch_list, points, -1)

    def group_share(item):
        group_raw, value_rows, weight_rows = item
        group = group_raw.astype(jnp.float32)
        obs_mean = lax.optimization_barrier(jnp.mean(group, axis=1))
        return build_transforms(group - obs_mean[:, None, :], value_rows - obs_mean, weight_rows)
    transform = lax.map(group_share, (ensemble, values, weights)).reshape(-1, members, members)
    share = stencil_weight / lax.optimization_barrier(jnp.sum(stencil_weight, axis=2, keepdims=True))
    total_cols = band_count * patch_list * columns
    block_cols = 16
    member_anomaly = state_pert.transpose(0, 1, 4, 2, 3).reshape(-1, block_cols, levels, members)
    index_cols = stencil.transpose(0, 1, 3, 2).reshape(-1, block_cols, 4)
    share_cols = share.transpose(0, 1, 3, 2).reshape(-1, block_cols, 4)

    def per_block(item):
        deviate, indices, portion = item
        merged_result = jnp.einsum('cs,cskl->ckl', portion, transform[indices], precision=largest_value)
        return jnp.einsum('cvk,ckl->cvl', deviate, merged_result, precision=largest_value)
    refreshed_state = lax.map(per_block, (member_anomaly, index_cols, share_cols)).reshape(total_cols, levels, members)
    mean_cols = state_mean.transpose(0, 1, 3, 2).reshape(total_cols, levels)
    refreshed_state = mean_cols[:, :, None] + refreshed_state
    per_device = block_target.shape[2]
    block_size = columns // per_device
    blocks = refreshed_state.reshape(band_count * patch_list * per_device, block_size, levels, members)
    targets = block_target.reshape(-1)
    native = jnp.zeros_like(blocks).at[targets].set(blocks)
    per_owner = band_count * per_device
    native = native.reshape(patch_list, per_owner, block_size, levels, members).transpose(0, 3, 4, 1, 2)
    return native.reshape(patch_list, levels, members, per_owner * block_size)
```

```python
import functools

import jax
import jax.numpy as jnp
from jax import lax
from jax.experimental import pallas as pl
from jax.experimental.pallas import tpu as pltpu
from jax.sharding import PartitionSpec as P

SWEEPS = 8
LANES = 128
CODE_TOP = 32700.0
LOG2E = 1.4426950408889634


largest_value = lax.Precision.HIGHEST
three_pass = lax.Precision.HIGH


def with_halo(block, sides, width):
    for axis, dim in sides:
        count = lax.axis_size(axis)
        forward = [(i, i + 1) for i in range(count - 1)]
        backward = [(target, source) for source, target in forward]
        low = lax.ppermute(
            lax.slice_in_dim(block, block.shape[dim] - width, None, axis=dim), axis, forward
        )
        high = lax.ppermute(lax.slice_in_dim(block, 0, width, axis=dim), axis, backward)
        block = jnp.concatenate([low, block, high], axis=dim)
    return block


def band_members(pieces, axis):
    count = lax.axis_size(axis)
    here = lax.axis_index(axis)
    arrived = []
    for step in range(count - 1, 0, -1):
        piece = lax.dynamic_index_in_dim(pieces, (here + step) % count, 0, keepdims=False)
        ring = [(i, (i + step) % count) for i in range(count)]
        arrived.append(lax.ppermute(piece, axis, ring))
    arrived.append(lax.dynamic_index_in_dim(pieces, here, 0, keepdims=False))
    width = arrived[0].shape[1]
    ringed = jnp.concatenate(arrived + arrived, axis=1)
    return lax.dynamic_slice_in_dim(ringed, (count - 1 - here) * width, count * width, axis=1)


def build_transforms(obs_pert, departure, obs_weight):
    scaled = obs_pert * obs_weight[:, None, :]
    gram_matrix = jnp.einsum("nko,nlo->nkl", scaled, obs_pert, precision=largest_value)
    forcing = jnp.einsum("nko,no->nk", scaled, departure, precision=largest_value)
    members = gram_matrix.shape[-1]
    identity = jnp.eye(members, dtype=jnp.float32)
    system = gram_matrix + (members - 1.0) * identity
    norm_sum = jnp.sqrt(jnp.sum(system * system, axis=(1, 2)))
    iterate = system / norm_sum[:, None, None]
    inverse = jnp.broadcast_to(identity, system.shape)
    for _ in range(SWEEPS):
        factor = 1.5 * identity - 0.5 * jnp.matmul(inverse, iterate, precision=three_pass)
        iterate = jnp.matmul(iterate, factor, precision=three_pass)
        inverse = jnp.matmul(factor, inverse, precision=three_pass)
    first_pass = jnp.einsum("nkl,nl->nk", inverse, forcing, precision=largest_value)
    mean_weight = (
        jnp.einsum("nkl,nl->nk", inverse, first_pass, precision=largest_value) / norm_sum[:, None]
    )
    spread = jnp.sqrt((members - 1.0) / norm_sum)[:, None, None] * inverse
    return spread + mean_weight[:, :, None]


def code_scale(exponent):
    return jnp.exp2(exponent) * (1.0 / CODE_TOP)


def column_kernel(
    from_ref, slot_ref, share_ref, states_ref, table_ref, out_ref, rows_ref, mix_ref, wide_ref,
    *, member_count, block_size, levels, members,
):
    owner = pl.program_id(0)
    first_column = from_ref[owner] * block_size
    width = members // member_count
    folds = max(1, LANES // width)
    rows = levels // folds
    rows_ref[...] = states_ref[...].astype(jnp.float32).reshape(members * block_size, levels)
    lane_group = lax.broadcasted_iota(jnp.int32, (rows, LANES), 1) // width
    strip = 64
    for i in range(block_size):
        column = first_column + i
        slots = [slot_ref[s, column] for s in range(4)]
        shares = [share_ref[s, column] for s in range(4)]
        buffer = i % 2
        for r in range(0, members, strip):
            mixed = shares[0] * table_ref[slots[0], r : r + strip, :]
            for s in range(1, 4):
                mixed = mixed + shares[s] * table_ref[slots[s], r : r + strip, :]
            high = mixed.astype(jnp.bfloat16)
            low = (mixed - high.astype(jnp.float32)).astype(jnp.bfloat16)
            mix_ref[buffer, r : r + strip, :members] = high
            mix_ref[buffer, r : r + strip, members:] = low
        state = rows_ref[pl.ds(i, members, stride=block_size), :].astype(jnp.bfloat16)
        both = lax.dot_general(
            state, mix_ref[buffer], (((0,), (0,)), ((), ())), preferred_element_type=jnp.float32
        )
        fresh = both[:, :members] + both[:, members:]
        for m in range(member_count):
            tile, offset = divmod(m * width, LANES)
            joined = None
            for h in range(folds):
                piece = fresh[h * rows : (h + 1) * rows, tile * LANES : (tile + 1) * LANES]
                shift = (h * width - offset) % LANES
                if shift:
                    piece = pltpu.roll(piece, shift, 1)
                joined = piece if joined is None else jnp.where(lane_group == h, piece, joined)
            wide_ref[m, pl.ds(i, rows, stride=block_size), :] = joined
    for m in range(member_count):
        values = wide_ref[m].reshape(rows, block_size, LANES)
        top = jnp.max(jnp.abs(values), axis=0)
        exponent = jnp.clip(jnp.ceil(jnp.log(top) * LOG2E), -100.0, 100.0)
        code = jnp.round(values * (1.0 / code_scale(exponent))[None])
        code = code.astype(jnp.int32).reshape(rows * block_size, LANES)
        out_ref[m, 0, : rows * block_size, :] = code.astype(jnp.int16)
        tail = jnp.concatenate([exponent, exponent], axis=0).astype(jnp.int32)
        out_ref[m, 0, rows * block_size :, :] = tail.astype(jnp.int16)


def columns_to_blocks(states, table, slots, share, send_from, member_count, block_size):
    members, columns, levels = states.shape
    patches = send_from.shape[0]
    width = members // member_count
    folds = max(1, LANES // width)
    rows = levels // folds
    coded = (rows + 2) * block_size
    kernel = functools.partial(
        column_kernel, member_count=member_count, block_size=block_size, levels=levels,
        members=members,
    )
    return pl.pallas_call(
        kernel,
        grid_spec=pltpu.PrefetchScalarGridSpec(
            num_scalar_prefetch=3,
            grid=(patches,),
            in_specs=[
                pl.BlockSpec((members, block_size, levels), lambda o, f, a, b: (0, f[o], 0)),
                pl.BlockSpec(table.shape, lambda o, f, a, b: (0, 0, 0)),
            ],
            out_specs=pl.BlockSpec(
                (member_count, 1, coded, LANES), lambda o, f, a, b: (0, o, 0, 0)
            ),
            scratch_shapes=[
                pltpu.VMEM((members * block_size, levels), jnp.float32),
                pltpu.VMEM((2, members, 2 * members), jnp.bfloat16),
                pltpu.VMEM((member_count, rows * block_size, LANES), jnp.float32),
            ],
        ),
        out_shape=jax.ShapeDtypeStruct((member_count, patches, coded, LANES), jnp.int16),
        cost_estimate=pl.CostEstimate(
            flops=4 * columns * levels * members * members, transcendentals=0,
            bytes_accessed=4 * states.size,
        ),
        name="columns",
    )(send_from, slots, share, states, table)


def native_kernel(source_ref, code_ref, tail_ref, out_ref, scale_ref, *, places, block_size):
    folds, pair, width, _ = out_ref.shape

    @pl.when(pl.program_id(0) == 0)
    def _():
        for t in range(places):
            tail = tail_ref[source_ref[t]].astype(jnp.int32).astype(jnp.float32)
            scale_ref[t] = code_scale(tail[:block_size])

    pieces = []
    for t in range(places):
        codes = code_ref[source_ref[t]].astype(jnp.int32).astype(jnp.float32)
        pieces.append((codes, scale_ref[t]))
    for r in range(pair):
        stacked = jnp.concatenate(
            [c[r * block_size : (r + 1) * block_size] * scale for c, scale in pieces], axis=0
        )
        out_ref[:, r] = stacked.T.reshape(folds, width, places * block_size)


def blocks_to_native(incoming, arrive_from, width, levels, block_size):
    sources, _, _ = incoming.shape
    places = arrive_from.shape[0]
    folds = max(1, LANES // width)
    rows = levels // folds
    pair = 2
    return pl.pallas_call(
        functools.partial(native_kernel, places=places, block_size=block_size),
        grid_spec=pltpu.PrefetchScalarGridSpec(
            num_scalar_prefetch=1,
            grid=(rows // pair,),
            in_specs=[
                pl.BlockSpec((sources, pair * block_size, LANES), lambda g, a: (0, g, 0)),
                pl.BlockSpec((sources, 2 * block_size, LANES), lambda g, a: (0, 0, 0)),
            ],
            out_specs=pl.BlockSpec(
                (folds, pair, width, places * block_size), lambda g, a: (0, g, 0, 0)
            ),
            scratch_shapes=[pltpu.VMEM((places, block_size, LANES), jnp.float32)],
        ),
        out_shape=jax.ShapeDtypeStruct((folds, rows, width, places * block_size), jnp.float32),
        name="native",
    )(arrive_from, incoming, incoming[:, rows * block_size :])


def analysis_shards(
    background, obs_ensemble, obs_value, obs_weight, stencil, stencil_weight, block_target
):
    own_obs = band_members(obs_ensemble[:, 0], "member")
    states = lax.all_to_all(
        background[:, 0].transpose(0, 2, 3, 1), "member", split_axis=0, concat_axis=0,
        tiled=True,
    )
    group = own_obs.astype(jnp.float32)
    obs_mean = jnp.mean(group, axis=1)
    transform = build_transforms(
        group - obs_mean[:, None, :], obs_value[0, 0] - obs_mean, obs_weight[0, 0]
    )
    points = transform.shape[0]
    members = transform.shape[1]
    transform = transform + (1.0 - jnp.sum(transform, axis=1, keepdims=True)) / members
    nearby = with_halo(transform[None, None], (("region", 1), ("member", 0)), 1)
    nearby = nearby.reshape(9 * points, members, members)
    columns, levels = states.shape[2:]
    states = states.reshape(members, columns, levels)
    band_index = lax.axis_index("member")
    patch_index = lax.axis_index("region")
    patch_list = lax.axis_size("region")
    member_count = lax.axis_size("member")
    shard_width = members // member_count
    stencil_rows = stencil[0, 0]
    near_band = stencil_rows // (patch_list * points)
    near_patch = stencil_rows // points % patch_list
    local_index = (
        (near_band - band_index + 1) * 3 + (near_patch - patch_index + 1)
    ) * points + stencil_rows % points
    share = stencil_weight[0, 0] / jnp.sum(stencil_weight[0, 0], axis=0, keepdims=True)
    band_count = block_target.shape[0]
    per_device = block_target.shape[2]
    per_owner = band_count * per_device
    block_size = columns // per_device
    owners = block_target // per_owner
    places = block_target % per_owner
    patch_ids = jnp.arange(patch_list, dtype=jnp.int32)
    place_ids = jnp.arange(per_owner, dtype=jnp.int32)
    band_owners = lax.dynamic_index_in_dim(owners, band_index, 0, keepdims=False)
    my_owners = lax.dynamic_index_in_dim(band_owners, patch_index, 0, keepdims=False)
    block_ids = jnp.arange(per_device, dtype=jnp.int32)
    send_hit = my_owners[None, :] == patch_ids[:, None]
    send_from = jnp.sum(send_hit.astype(jnp.int32) * block_ids[None, :], axis=1)
    band_ids = jnp.arange(band_count, dtype=jnp.int32)
    source = band_ids[:, None, None] * patch_list + patch_ids[None, :, None] + 0 * places
    arrive_hit = (owners == patch_index)[None] & (places[None] == place_ids[:, None, None, None])
    arrive_from = jnp.sum(arrive_hit.astype(jnp.int32) * source[None], axis=(1, 2, 3))
    outgoing = columns_to_blocks(
        states, nearby, local_index, share, send_from, member_count, block_size
    )
    outgoing = outgoing.reshape(member_count * patch_list, *outgoing.shape[2:])
    incoming = lax.all_to_all(
        outgoing, ("member", "region"), split_axis=0, concat_axis=0, tiled=True
    )
    native = blocks_to_native(incoming, arrive_from, shard_width, levels, block_size)
    return native.reshape(1, levels, shard_width, per_owner * block_size)


def solution(mesh):
    in_specs = (
        P(None, "region", None, "member", None),
        P(None, "region", None, "member", None),
        P("member", "region", None, None),
        P("member", "region", None, None),
        P("member", "region", None, None),
        P("member", "region", None, None),
        P(),
    )
    out_specs = P("region", None, "member", None)
    return jax.shard_map(analysis_shards, mesh=mesh, in_specs=in_specs, out_specs=out_specs, check_vma=False)
```

```python
import functools
import math

import jax
import jax.numpy as jnp
from jax import lax
from jax.experimental import pallas as pl
from jax.experimental.pallas import tpu as pltpu
from jax.sharding import PartitionSpec as P

SWEEPS = 8
LANES = 128
CODE_TOP = 32700.0
LOG2E = 1.4426950408889634


def halo_pair(block, axis):
    count = lax.axis_size(axis)
    forward = [(i, i + 1) for i in range(count - 1)]
    backward = [(target, source) for source, target in forward]
    return lax.ppermute(block, axis, forward), lax.ppermute(block, axis, backward)


def band_members(pieces, axis):
    count = lax.axis_size(axis)
    here = lax.axis_index(axis)
    arrived = []
    for step in range(count - 1, 0, -1):
        piece = lax.dynamic_index_in_dim(pieces, (here + step) % count, 0, keepdims=False)
        ring = [(i, (i + step) % count) for i in range(count)]
        arrived.append(lax.ppermute(piece, axis, ring))
    return arrived


def halves(value):
    high = value.astype(jnp.bfloat16)
    return high, (value - high.astype(jnp.float32)).astype(jnp.bfloat16)


def product(left, right, contract=((1,), (0,))):
    def one(a, b):
        return lax.dot_general(a, b, (contract, ((), ())), preferred_element_type=jnp.float32)

    return one(left[0], right[0]) + (one(left[0], right[1]) + one(left[1], right[0]))


def transform_kernel(here_ref, value_ref, weight_ref, own_ref, *refs, member_count, fill):
    arrived, code_ref, group_ref = refs[:-2], refs[-2], refs[-1]
    width = own_ref.shape[2]
    members = member_count * width
    here = here_ref[0]
    group_ref[pl.ds(pl.multiple_of(here * width, width), width), :] = own_ref[0, 0].astype(
        jnp.float32
    )
    for i, piece in enumerate(arrived):
        source = (here + 1 + i) % member_count
        group_ref[pl.ds(pl.multiple_of(source * width, width), width), :] = piece[0].astype(
            jnp.float32
        )
    group = group_ref[...]
    mean = jnp.sum(group, axis=0, keepdims=True) * (1.0 / members)
    pert = group - mean
    departure = value_ref[0] - mean
    scaled = pert * weight_ref[0]
    gram = product(halves(scaled), halves(pert), ((1,), (1,)))
    forcing = jnp.sum(scaled * departure, axis=1, keepdims=True)
    rows_at = lax.broadcasted_iota(jnp.int32, (members, members), 0)
    columns_at = lax.broadcasted_iota(jnp.int32, (members, members), 1)
    identity = (rows_at == columns_at).astype(jnp.float32)
    system = gram + (members - 1.0) * identity
    norm = jnp.sqrt(
        jnp.sum(jnp.sum(system * system, axis=1, keepdims=True), axis=0, keepdims=True)
    )
    iterate = system / norm
    factor = 1.5 * identity - 0.5 * iterate
    inverse = factor
    iterate = product(halves(iterate), halves(factor))
    for sweep in range(1, SWEEPS):
        inverse_halves = halves(inverse)
        iterate_halves = halves(iterate)
        factor = 1.5 * identity - 0.5 * product(inverse_halves, iterate_halves)
        factor_halves = halves(factor)
        if sweep < SWEEPS - 1:
            iterate = product(iterate_halves, factor_halves)
        inverse = product(factor_halves, inverse_halves)
    first = jnp.sum(inverse * forcing, axis=0, keepdims=True)
    mean_weight = jnp.sum(inverse * first, axis=1, keepdims=True) / norm
    transform = jnp.sqrt((members - 1.0) / norm) * inverse + mean_weight
    total = jnp.sum(transform, axis=0, keepdims=True)
    transform = transform + (1.0 - total) * (1.0 / members)
    inner = width // fill
    transform = jnp.concatenate(
        [
            transform[(m * fill + q) * inner :][:inner]
            for q in range(fill)
            for m in range(member_count)
        ],
        axis=0,
    )
    values = transform.reshape(members // 8, 8, members)
    exponent = code_exponent(values)
    code = jnp.round(values * (1.0 / code_scale(exponent))[None])
    code_ref[0, :members, :] = code.astype(jnp.int32).reshape(members, members).astype(jnp.int16)
    tail = jnp.concatenate([exponent, exponent], axis=0).astype(jnp.int32)
    code_ref[0, members:, :] = tail.astype(jnp.int16)


def coded_transforms(obs_ensemble, obs_value, obs_weight, fill):
    member_count, points, width, observations = obs_ensemble.shape
    members = member_count * width
    here = lax.axis_index("member").astype(jnp.int32).reshape(1)
    arrived = band_members(obs_ensemble, "member")
    line = pl.BlockSpec((1, 1, observations), lambda n, h: (n, 0, 0))
    return pl.pallas_call(
        functools.partial(transform_kernel, member_count=member_count, fill=fill),
        grid_spec=pltpu.PrefetchScalarGridSpec(
            num_scalar_prefetch=1,
            grid=(points,),
            in_specs=[
                line,
                line,
                pl.BlockSpec((1, 1, width, observations), lambda n, h: (h[0], n, 0, 0)),
            ]
            + [pl.BlockSpec((1, width, observations), lambda n, h: (n, 0, 0))] * len(arrived),
            out_specs=pl.BlockSpec((1, members + 16, members), lambda n, h: (n, 0, 0)),
            scratch_shapes=[pltpu.VMEM((members, observations), jnp.float32)],
        ),
        out_shape=jax.ShapeDtypeStruct((points, members + 16, members), jnp.int16),
        name="transforms",
    )(here, obs_value[:, None], obs_weight[:, None], obs_ensemble, *arrived)


def code_exponent(values):
    top = jnp.max(jnp.abs(values), axis=0)
    return jnp.clip(jnp.ceil(jnp.log(top) * LOG2E), -100.0, 100.0)


def code_scale(exponent):
    return jnp.exp2(exponent) * (1.0 / CODE_TOP)


def pack_kernel(order_ref, states_ref, first_ref, second_ref, *, group):
    _, width, columns, levels = states_ref.shape
    fill = LANES // group
    inner = width // fill
    cut = first_ref.shape[1]
    lane_group = lax.broadcasted_iota(jnp.int32, (columns, LANES), 1) // group
    spare = jnp.zeros((columns, -levels % LANES), jnp.float32)
    for r in range(inner):
        source = [
            jnp.concatenate([states_ref[0, q * inner + r].astype(jnp.float32), spare], axis=1)
            for q in range(fill)
        ]
        for g in range(levels // group):
            tile, offset = divmod(g * group, LANES)
            joined = None
            for q in range(fill):
                piece = source[q][:, tile * LANES : (tile + 1) * LANES]
                shift = (q * group - offset) % LANES
                if shift:
                    piece = pltpu.roll(piece, shift, 1)
                joined = piece if joined is None else jnp.where(lane_group == q, piece, joined)
            if g < cut:
                first_ref[0, g, r] = joined.astype(jnp.bfloat16)
            else:
                second_ref[0, g - cut, r] = joined.astype(jnp.bfloat16)


def pack_lanes(states, order, cut):
    bands, width, columns, levels = states.shape
    group = math.gcd(levels, LANES)
    inner = width * group // LANES
    shapes = [(count, inner, columns, LANES) for count in (cut, levels // group - cut)]
    return pl.pallas_call(
        functools.partial(pack_kernel, group=group),
        grid_spec=pltpu.PrefetchScalarGridSpec(
            num_scalar_prefetch=1,
            grid=(bands,),
            in_specs=[pl.BlockSpec((1, width, columns, levels), lambda b, o: (o[b], 0, 0, 0))],
            out_specs=[
                pl.BlockSpec((1, *shapes[0]), lambda b, o: (o[b], 0, 0, 0, 0)),
                pl.BlockSpec((1, *shapes[1]), lambda b, o: (b, 0, 0, 0, 0)),
            ],
        ),
        out_shape=[jax.ShapeDtypeStruct((bands, *shape), jnp.bfloat16) for shape in shapes],
        name="pack",
    )(order, states)


def column_kernel(
    from_ref, slot_ref, share_ref, source_ref, *refs, member_count, block_size, levels, members,
    group,
):
    states_refs = refs[:-8]
    low_ref, own_ref, high_ref, out_ref, table_ref, rows_ref, mix_ref, wide_ref = refs[-8:]
    owner = pl.program_id(0)

    @pl.when(owner == 0)
    def _():
        for side, side_ref in enumerate((low_ref, own_ref, high_ref)):
            tiles = side_ref.shape[0]
            for n in range(tiles):
                tail = side_ref[n, members:, :].astype(jnp.int32).astype(jnp.float32)
                scale = code_scale(tail[:8])[None]

                def decode(r, carry):
                    start = pl.multiple_of(r * 64, 64)
                    code = side_ref[n, pl.ds(start, 64), :].astype(jnp.int32).astype(jnp.float32)
                    value = code.reshape(8, 8, members) * scale
                    table_ref[side * tiles + n, pl.ds(start, 64), :] = value.reshape(64, members)
                    return carry

                lax.fori_loop(0, members // 64, decode, 0)

    first_column = from_ref[owner] * block_size
    width = members // member_count
    folds = max(1, LANES // width)
    rows = levels // folds
    fill = LANES // group
    groups = levels // group
    inner = width // fill
    packed = member_count * groups * inner
    for n, states_ref in enumerate(states_refs):
        height = states_ref.shape[0] * block_size
        start = pl.multiple_of(source_ref[n] * height, height)
        rows_ref[pl.ds(start, height), :] = (
            states_ref[...].astype(jnp.float32).reshape(height, LANES)
        )
    lane_group = lax.broadcasted_iota(jnp.int32, (rows, LANES), 1) // width
    strip = 32
    for i in range(block_size):
        column = first_column + i
        slots = [slot_ref[s, column] for s in range(4)]
        shares = [share_ref[s, column] for s in range(4)]
        buffer = i % 2
        for r in range(0, members, strip):
            mixed = shares[0] * table_ref[slots[0], r : r + strip, :]
            for s in range(1, 4):
                mixed = mixed + shares[s] * table_ref[slots[s], r : r + strip, :]
            high = mixed.astype(jnp.bfloat16)
            low = (mixed - high.astype(jnp.float32)).astype(jnp.bfloat16)
            mix_ref[buffer, r : r + strip, :] = high
            mix_ref[buffer, members + r : members + r + strip, :] = low
        dense = rows_ref[pl.ds(i, packed, stride=block_size), :]
        lines = []
        for g in range(groups):
            part = jnp.concatenate(
                [dense[(m * groups + g) * inner :][:inner] for m in range(member_count)], axis=0
            )
            turned = part.astype(jnp.bfloat16).T
            lines.append(
                jnp.concatenate([turned[q * group : (q + 1) * group] for q in range(fill)], axis=1)
            )
        state = jnp.concatenate(lines, axis=0)
        fresh = jnp.dot(
            jnp.concatenate([state, state], axis=1), mix_ref[buffer],
            preferred_element_type=jnp.float32,
        )
        for m in range(member_count):
            tile, offset = divmod(m * width, LANES)
            joined = None
            for h in range(folds):
                piece = jnp.concatenate(
                    [fresh[(t * folds + h) * 8 :][:8] for t in range(rows // 8)], axis=0
                )[:, tile * LANES : (tile + 1) * LANES]
                shift = (h * width - offset) % LANES
                if shift:
                    piece = pltpu.roll(piece, shift, 1)
                joined = piece if joined is None else jnp.where(lane_group == h, piece, joined)
            wide_ref[m, pl.ds(i, rows, stride=block_size), :] = joined
    for m in range(member_count):
        values = wide_ref[m].reshape(rows, block_size, LANES)
        exponent = code_exponent(values)
        code = jnp.round(values * (1.0 / code_scale(exponent))[None])
        code = code.astype(jnp.int32).reshape(rows * block_size, LANES)
        out_ref[m, 0, : rows * block_size, :] = code.astype(jnp.int16)
        out_ref[m, 0, rows * block_size :, :] = exponent.astype(jnp.int32).astype(jnp.int16)


def columns_to_blocks(
    states, source, sides, slots, share, send_from, group, levels, member_count, block_size
):
    tiles, _, members = sides[0].shape
    columns = states[0].shape[1]
    patches = send_from.shape[0]
    packed = sum(piece.shape[0] for piece in states)
    width = members // member_count
    folds = max(1, LANES // width)
    rows = levels // folds
    coded = (rows + 1) * block_size
    kernel = functools.partial(
        column_kernel, member_count=member_count, block_size=block_size, levels=levels,
        members=members, group=group,
    )
    return pl.pallas_call(
        kernel,
        grid_spec=pltpu.PrefetchScalarGridSpec(
            num_scalar_prefetch=4,
            grid=(patches,),
            in_specs=[
                pl.BlockSpec((piece.shape[0], block_size, LANES), lambda o, f, a, b, c: (0, f[o], 0))
                for piece in states
            ]
            + [pl.BlockSpec(sides[0].shape, lambda o, f, a, b, c: (0, 0, 0))] * len(sides),
            out_specs=pl.BlockSpec(
                (member_count, 1, coded, LANES), lambda o, f, a, b, c: (0, o, 0, 0)
            ),
            scratch_shapes=[
                pltpu.VMEM((len(sides) * tiles, members, members), jnp.float32),
                pltpu.VMEM((packed * block_size, LANES), jnp.float32),
                pltpu.VMEM((2, 2 * members, members), jnp.bfloat16),
                pltpu.VMEM((member_count, rows * block_size, LANES), jnp.float32),
            ],
        ),
        out_shape=jax.ShapeDtypeStruct((member_count, patches, coded, LANES), jnp.int16),
        cost_estimate=pl.CostEstimate(
            flops=4 * columns * levels * members * members, transcendentals=0,
            bytes_accessed=4 * packed * columns * LANES,
        ),
        name="columns",
    )(send_from, slots, share, source, *states, *sides)


def native_kernel(source_ref, code_ref, *refs, places, block_size, tail_at):
    out_ref, scale_ref = refs[-2:]
    height, width, _ = out_ref.shape
    folds = max(1, LANES // width)
    strip = height // folds
    pair = 2 * block_size

    @pl.when(pl.program_id(0) == 0)
    def _():
        for t in range(places):
            tail = code_ref[source_ref[t], tail_at : tail_at + block_size, :]
            scale_ref[t] = code_scale(tail.astype(jnp.int32).astype(jnp.float32))

    first = pl.program_id(0) * (strip * block_size)
    for r in range(0, strip, 2):
        start = pl.multiple_of(first + r * block_size, pair)
        pieces = [
            code_ref[source_ref[t], pl.ds(start, pair), :].astype(jnp.int32).astype(jnp.float32)
            for t in range(places)
        ]
        for half in range(2):
            stacked = jnp.concatenate(
                [
                    piece[half * block_size : (half + 1) * block_size] * scale_ref[t]
                    for t, piece in enumerate(pieces)
                ],
                axis=0,
            )
            turned = stacked.T
            for h in range(folds):
                out_ref[h * strip + r + half] = turned[h * width : (h + 1) * width]


def blocks_to_native(incoming, arrive_from, previous, width, levels, from_level, block_size):
    _, coded, _ = incoming.shape
    places = arrive_from.shape[0]
    folds = max(1, LANES // width)
    tail_at = coded - block_size
    height = 8 * folds
    first = from_level // height
    return pl.pallas_call(
        functools.partial(native_kernel, places=places, block_size=block_size, tail_at=tail_at),
        grid_spec=pltpu.PrefetchScalarGridSpec(
            num_scalar_prefetch=1,
            grid=(tail_at // block_size // 8,),
            in_specs=[pl.BlockSpec(memory_space=pltpu.VMEM)]
            + [pl.BlockSpec(memory_space=pl.ANY)] * len(previous),
            out_specs=pl.BlockSpec(
                (height, width, places * block_size), lambda g, a: (first + g, 0, 0)
            ),
            scratch_shapes=[pltpu.VMEM((places, block_size, LANES), jnp.float32)],
        ),
        out_shape=jax.ShapeDtypeStruct((levels, width, places * block_size), jnp.float32),
        input_output_aliases={2: 0} if previous else {},
        name="native",
    )(arrive_from, incoming, *previous)


def analysis_shards(
    background, obs_ensemble, obs_value, obs_weight, stencil, stencil_weight, block_target
):
    members = obs_ensemble.shape[3] * lax.axis_size("member")
    fill = LANES // math.gcd(background.shape[2], LANES)
    coded = coded_transforms(obs_ensemble[:, 0], obs_value[0, 0], obs_weight[0, 0], fill)
    points = coded.shape[0]
    member_count = lax.axis_size("member")
    band_index = lax.axis_index("member")
    levels, columns = background.shape[2], background.shape[4]
    group = math.gcd(levels, LANES)
    groups = levels // group
    cut = max(1, groups // 3)
    order = (band_index + jnp.arange(member_count, dtype=jnp.int32)) % member_count
    early, late = pack_lanes(background[:, 0].transpose(0, 2, 3, 1), order, cut)
    early = lax.all_to_all(early, "member", split_axis=0, concat_axis=0, tiled=True)
    late = [late[step] for step in range(member_count)]
    left, right = halo_pair(coded, "region")
    left, *late = lax.optimization_barrier((left, *late))
    trio = jnp.concatenate([left, coded, right], axis=0)
    low, high = halo_pair(trio, "member")
    late_pieces = [late[0].reshape(-1, columns, LANES)]
    for step in range(1, member_count):
        ring = [(i, (i + step) % member_count) for i in range(member_count)]
        arrived = lax.ppermute(late[step], "member", ring)
        late_pieces.append(arrived.reshape(-1, columns, LANES))
    late_source = (band_index - jnp.arange(member_count, dtype=jnp.int32)) % member_count
    early_source = jnp.zeros((1,), jnp.int32)
    patch_index = lax.axis_index("region")
    patch_list = lax.axis_size("region")
    shard_width = members // member_count
    stencil_rows = stencil[0, 0]
    near_band = stencil_rows // (patch_list * points)
    near_patch = stencil_rows // points % patch_list
    local_index = (
        (near_band - band_index + 1) * 3 + (near_patch - patch_index + 1)
    ) * points + stencil_rows % points
    share = stencil_weight[0, 0] / jnp.sum(stencil_weight[0, 0], axis=0, keepdims=True)
    band_count = block_target.shape[0]
    per_device = block_target.shape[2]
    per_owner = band_count * per_device
    block_size = columns // per_device
    owners = block_target // per_owner
    places = block_target % per_owner
    patch_ids = jnp.arange(patch_list, dtype=jnp.int32)
    place_ids = jnp.arange(per_owner, dtype=jnp.int32)
    band_owners = lax.dynamic_index_in_dim(owners, band_index, 0, keepdims=False)
    my_owners = lax.dynamic_index_in_dim(band_owners, patch_index, 0, keepdims=False)
    block_ids = jnp.arange(per_device, dtype=jnp.int32)
    send_hit = my_owners[None, :] == patch_ids[:, None]
    send_from = jnp.sum(send_hit.astype(jnp.int32) * block_ids[None, :], axis=1)
    band_ids = jnp.arange(band_count, dtype=jnp.int32)
    source = band_ids[:, None, None] * patch_list + patch_ids[None, :, None] + 0 * places
    arrive_hit = (owners == patch_index)[None] & (places[None] == place_ids[:, None, None, None])
    arrive_from = jnp.sum(arrive_hit.astype(jnp.int32) * source[None], axis=(1, 2, 3))
    native = ()
    chunks = (
        (0, cut, [early.reshape(-1, columns, LANES)], early_source),
        (cut, groups, late_pieces, late_source),
    )
    for start, end, states, state_source in chunks:
        outgoing = columns_to_blocks(
            states, state_source, (low, trio, high), local_index, share, send_from, group,
            (end - start) * group, member_count, block_size,
        )
        outgoing = outgoing.reshape(member_count * patch_list, *outgoing.shape[2:])
        incoming = lax.all_to_all(
            outgoing, ("member", "region"), split_axis=0, concat_axis=0, tiled=True
        )
        native = (
            blocks_to_native(
                incoming, arrive_from, native, shard_width, levels, start * group, block_size
            ),
        )
    return native[0].reshape(1, levels, shard_width, per_owner * block_size)


def solution(mesh):
    in_specs = (
        P(None, "region", None, "member", None),
        P(None, "region", None, "member", None),
        P("member", "region", None, None),
        P("member", "region", None, None),
        P("member", "region", None, None),
        P("member", "region", None, None),
        P(),
    )
    out_specs = P("region", None, "member", None)
    return jax.shard_map(analysis_shards, mesh=mesh, in_specs=in_specs, out_specs=out_specs, check_vma=False)
```

```python
import functools
import math

import jax
import jax.numpy as jnp
from jax import lax
from jax.experimental import pallas as pl
from jax.experimental.pallas import tpu as pltpu
from jax.sharding import PartitionSpec as P

SWEEPS = 8
LANES = 128
CODE_TOP = 32700.0
LOG2E = 1.4426950408889634


def halo_pair(block, axis):
    count = lax.axis_size(axis)
    forward = [(i, i + 1) for i in range(count - 1)]
    backward = [(target, source) for source, target in forward]
    return lax.ppermute(block, axis, forward), lax.ppermute(block, axis, backward)


def band_members(pieces, axis):
    count = lax.axis_size(axis)
    here = lax.axis_index(axis)
    arrived = []
    for step in range(count - 1, 0, -1):
        piece = lax.dynamic_index_in_dim(pieces, (here + step) % count, 0, keepdims=False)
        ring = [(i, (i + step) % count) for i in range(count)]
        arrived.append(lax.ppermute(piece, axis, ring))
    return arrived


def halves(value):
    high = value.astype(jnp.bfloat16)
    return high, (value - high.astype(jnp.float32)).astype(jnp.bfloat16)


def product(left, right, contract=((1,), (0,))):
    def one(a, b):
        return lax.dot_general(a, b, (contract, ((), ())), preferred_element_type=jnp.float32)

    return one(left[0], right[0]) + (one(left[0], right[1]) + one(left[1], right[0]))


def transform_kernel(here_ref, value_ref, weight_ref, own_ref, *refs, member_count, fill):
    arrived, code_ref, group_ref = refs[:-2], refs[-2], refs[-1]
    width = own_ref.shape[2]
    members = member_count * width
    here = here_ref[0]
    group_ref[pl.ds(pl.multiple_of(here * width, width), width), :] = own_ref[0, 0].astype(
        jnp.float32
    )
    for i, piece in enumerate(arrived):
        source = (here + 1 + i) % member_count
        group_ref[pl.ds(pl.multiple_of(source * width, width), width), :] = piece[0].astype(
            jnp.float32
        )
    group = group_ref[...]
    mean = jnp.sum(group, axis=0, keepdims=True) * (1.0 / members)
    pert = group - mean
    departure = value_ref[0] - mean
    scaled = pert * weight_ref[0]
    gram = product(halves(scaled), halves(pert), ((1,), (1,)))
    forcing = jnp.sum(scaled * departure, axis=1, keepdims=True)
    rows_at = lax.broadcasted_iota(jnp.int32, (members, members), 0)
    columns_at = lax.broadcasted_iota(jnp.int32, (members, members), 1)
    identity = (rows_at == columns_at).astype(jnp.float32)
    system = gram + (members - 1.0) * identity
    norm = jnp.sqrt(
        jnp.sum(jnp.sum(system * system, axis=1, keepdims=True), axis=0, keepdims=True)
    )
    iterate = system / norm
    factor = 1.5 * identity - 0.5 * iterate
    inverse = factor
    iterate = product(halves(iterate), halves(factor))
    for sweep in range(1, SWEEPS):
        inverse_halves = halves(inverse)
        iterate_halves = halves(iterate)
        factor = 1.5 * identity - 0.5 * product(inverse_halves, iterate_halves)
        factor_halves = halves(factor)
        if sweep < SWEEPS - 1:
            iterate = product(iterate_halves, factor_halves)
        inverse = product(factor_halves, inverse_halves)
    first = jnp.sum(inverse * forcing, axis=0, keepdims=True)
    mean_weight = jnp.sum(inverse * first, axis=1, keepdims=True) / norm
    transform = jnp.sqrt((members - 1.0) / norm) * inverse + mean_weight
    total = jnp.sum(transform, axis=0, keepdims=True)
    transform = transform + (1.0 - total) * (1.0 / members)
    inner = width // fill
    transform = jnp.concatenate(
        [
            transform[(m * fill + q) * inner :][:inner]
            for q in range(fill)
            for m in range(member_count)
        ],
        axis=0,
    )
    values = transform.reshape(members // 8, 8, members)
    exponent = code_exponent(values)
    code = jnp.round(values * (1.0 / code_scale(exponent))[None])
    code_ref[0, :members, :] = code.astype(jnp.int32).reshape(members, members).astype(jnp.int16)
    code_ref[0, members:, :] = exponent.astype(jnp.int32).astype(jnp.int16)


def coded_transforms(obs_ensemble, obs_value, obs_weight, fill):
    member_count, points, width, observations = obs_ensemble.shape
    members = member_count * width
    here = lax.axis_index("member").astype(jnp.int32).reshape(1)
    arrived = band_members(obs_ensemble, "member")
    line = pl.BlockSpec((1, 1, observations), lambda n, h: (n, 0, 0))
    return pl.pallas_call(
        functools.partial(transform_kernel, member_count=member_count, fill=fill),
        grid_spec=pltpu.PrefetchScalarGridSpec(
            num_scalar_prefetch=1,
            grid=(points,),
            in_specs=[
                line,
                line,
                pl.BlockSpec((1, 1, width, observations), lambda n, h: (h[0], n, 0, 0)),
            ]
            + [pl.BlockSpec((1, width, observations), lambda n, h: (n, 0, 0))] * len(arrived),
            out_specs=pl.BlockSpec((1, members + 8, members), lambda n, h: (n, 0, 0)),
            scratch_shapes=[pltpu.VMEM((members, observations), jnp.float32)],
        ),
        out_shape=jax.ShapeDtypeStruct((points, members + 8, members), jnp.int16),
        name="transforms",
    )(here, obs_value[:, None], obs_weight[:, None], obs_ensemble, *arrived)


def code_exponent(values):
    top = jnp.max(jnp.abs(values), axis=0)
    return jnp.clip(jnp.ceil(jnp.log(top) * LOG2E), -100.0, 100.0)


def code_scale(exponent):
    return jnp.exp2(exponent) * (1.0 / CODE_TOP)


def pack_kernel(order_ref, states_ref, first_ref, second_ref, *, group):
    _, width, columns, levels = states_ref.shape
    fill = LANES // group
    inner = width // fill
    cut = first_ref.shape[1]
    lane_group = lax.broadcasted_iota(jnp.int32, (columns, LANES), 1) // group
    spare = jnp.zeros((columns, -levels % LANES), jnp.float32)
    for r in range(inner):
        source = [
            jnp.concatenate([states_ref[0, q * inner + r].astype(jnp.float32), spare], axis=1)
            for q in range(fill)
        ]
        for g in range(levels // group):
            tile, offset = divmod(g * group, LANES)
            joined = None
            for q in range(fill):
                piece = source[q][:, tile * LANES : (tile + 1) * LANES]
                shift = (q * group - offset) % LANES
                if shift:
                    piece = pltpu.roll(piece, shift, 1)
                joined = piece if joined is None else jnp.where(lane_group == q, piece, joined)
            if g < cut:
                first_ref[0, g, r] = joined.astype(jnp.bfloat16)
            else:
                second_ref[0, g - cut, r] = joined.astype(jnp.bfloat16)


def pack_lanes(states, order, cut):
    bands, width, columns, levels = states.shape
    group = math.gcd(levels, LANES)
    inner = width * group // LANES
    shapes = [(count, inner, columns, LANES) for count in (cut, levels // group - cut)]
    return pl.pallas_call(
        functools.partial(pack_kernel, group=group),
        grid_spec=pltpu.PrefetchScalarGridSpec(
            num_scalar_prefetch=1,
            grid=(bands,),
            in_specs=[pl.BlockSpec((1, width, columns, levels), lambda b, o: (o[b], 0, 0, 0))],
            out_specs=[
                pl.BlockSpec((1, *shapes[0]), lambda b, o: (o[b], 0, 0, 0, 0)),
                pl.BlockSpec((1, *shapes[1]), lambda b, o: (b, 0, 0, 0, 0)),
            ],
        ),
        out_shape=[jax.ShapeDtypeStruct((bands, *shape), jnp.bfloat16) for shape in shapes],
        name="pack",
    )(order, states)


def column_kernel(
    from_ref, slot_ref, share_ref, source_ref, *refs, member_count, block_size, levels, members,
    group,
):
    states_refs = refs[:-8]
    low_ref, own_ref, high_ref, out_ref, table_ref, rows_ref, mix_ref, wide_ref = refs[-8:]
    owner = pl.program_id(0)

    @pl.when(owner == 0)
    def _():
        for side, side_ref in enumerate((low_ref, own_ref, high_ref)):
            tiles = side_ref.shape[0]
            for n in range(tiles):
                tail = side_ref[n, members:, :].astype(jnp.int32).astype(jnp.float32)
                scale = code_scale(tail)[None]

                def decode(r, carry):
                    start = pl.multiple_of(r * 64, 64)
                    code = side_ref[n, pl.ds(start, 64), :].astype(jnp.int32).astype(jnp.float32)
                    value = code.reshape(8, 8, members) * scale
                    table_ref[side * tiles + n, pl.ds(start, 64), :] = value.reshape(64, members)
                    return carry

                lax.fori_loop(0, members // 64, decode, 0, unroll=True)

    first_column = from_ref[owner] * block_size
    width = members // member_count
    folds = max(1, LANES // width)
    rows = levels // folds
    fill = LANES // group
    groups = levels // group
    inner = width // fill
    packed = member_count * groups * inner
    for n, states_ref in enumerate(states_refs):
        height = states_ref.shape[0] * block_size
        start = pl.multiple_of(source_ref[n] * height, height)
        rows_ref[pl.ds(start, height), :] = (
            states_ref[...].astype(jnp.float32).reshape(height, LANES)
        )
    lane_group = lax.broadcasted_iota(jnp.int32, (rows, LANES), 1) // width
    strip = 32
    for i in range(block_size):
        column = first_column + i
        slots = [slot_ref[s, column] for s in range(4)]
        shares = [share_ref[s, column] for s in range(4)]
        buffer = i % 2
        for r in range(0, members, strip):
            mixed = shares[0] * table_ref[slots[0], r : r + strip, :]
            for s in range(1, 4):
                mixed = mixed + shares[s] * table_ref[slots[s], r : r + strip, :]
            high = mixed.astype(jnp.bfloat16)
            low = (mixed - high.astype(jnp.float32)).astype(jnp.bfloat16)
            mix_ref[buffer, r : r + strip, :] = high
            mix_ref[buffer, members + r : members + r + strip, :] = low
        dense = rows_ref[pl.ds(i, packed, stride=block_size), :]
        lines = []
        for g in range(groups):
            part = jnp.concatenate(
                [dense[(m * groups + g) * inner :][:inner] for m in range(member_count)], axis=0
            )
            turned = part.astype(jnp.bfloat16).T
            lines.append(
                jnp.concatenate([turned[q * group : (q + 1) * group] for q in range(fill)], axis=1)
            )
        state = jnp.concatenate(lines, axis=0)
        fresh = jnp.dot(
            jnp.concatenate([state, state], axis=1), mix_ref[buffer],
            preferred_element_type=jnp.float32,
        )
        for m in range(member_count):
            tile, offset = divmod(m * width, LANES)
            joined = None
            for h in range(folds):
                piece = jnp.concatenate(
                    [fresh[(t * folds + h) * 8 :][:8] for t in range(rows // 8)], axis=0
                )[:, tile * LANES : (tile + 1) * LANES]
                shift = (h * width - offset) % LANES
                if shift:
                    piece = pltpu.roll(piece, shift, 1)
                joined = piece if joined is None else jnp.where(lane_group == h, piece, joined)
            wide_ref[m, pl.ds(i, rows, stride=block_size), :] = joined
    for m in range(member_count):
        values = wide_ref[m].reshape(rows, block_size, LANES)
        exponent = code_exponent(values)
        code = jnp.round(values * (1.0 / code_scale(exponent))[None])
        code = code.astype(jnp.int32).reshape(rows * block_size, LANES)
        out_ref[m, 0, : rows * block_size, :] = code.astype(jnp.int16)
        out_ref[m, 0, rows * block_size :, :] = exponent.astype(jnp.int32).astype(jnp.int16)


def columns_to_blocks(
    states, source, sides, slots, share, send_from, group, levels, member_count, block_size
):
    tiles, _, members = sides[0].shape
    columns = states[0].shape[1]
    patches = send_from.shape[0]
    packed = sum(piece.shape[0] for piece in states)
    width = members // member_count
    folds = max(1, LANES // width)
    rows = levels // folds
    coded = (rows + 1) * block_size
    kernel = functools.partial(
        column_kernel, member_count=member_count, block_size=block_size, levels=levels,
        members=members, group=group,
    )
    return pl.pallas_call(
        kernel,
        grid_spec=pltpu.PrefetchScalarGridSpec(
            num_scalar_prefetch=4,
            grid=(patches,),
            in_specs=[
                pl.BlockSpec((piece.shape[0], block_size, LANES), lambda o, f, a, b, c: (0, f[o], 0))
                for piece in states
            ]
            + [pl.BlockSpec(sides[0].shape, lambda o, f, a, b, c: (0, 0, 0))] * len(sides),
            out_specs=pl.BlockSpec(
                (member_count, 1, coded, LANES), lambda o, f, a, b, c: (0, o, 0, 0)
            ),
            scratch_shapes=[
                pltpu.VMEM((len(sides) * tiles, members, members), jnp.float32),
                pltpu.VMEM((packed * block_size, LANES), jnp.float32),
                pltpu.VMEM((2, 2 * members, members), jnp.bfloat16),
                pltpu.VMEM((member_count, rows * block_size, LANES), jnp.float32),
            ],
        ),
        out_shape=jax.ShapeDtypeStruct((member_count, patches, coded, LANES), jnp.int16),
        cost_estimate=pl.CostEstimate(
            flops=4 * columns * levels * members * members, transcendentals=0,
            bytes_accessed=4 * packed * columns * LANES,
        ),
        name="columns",
    )(send_from, slots, share, source, *states, *sides)


def native_kernel(source_ref, code_ref, *refs, places, block_size, tail_at):
    out_ref, scale_ref = refs[-2:]
    height, width, _ = out_ref.shape
    folds = max(1, LANES // width)
    strip = height // folds
    pair = 2 * block_size

    @pl.when(pl.program_id(0) == 0)
    def _():
        for t in range(places):
            tail = code_ref[source_ref[t], tail_at : tail_at + block_size, :]
            scale_ref[t] = code_scale(tail.astype(jnp.int32).astype(jnp.float32))

    first = pl.program_id(0) * (strip * block_size)
    for r in range(0, strip, 2):
        start = pl.multiple_of(first + r * block_size, pair)
        pieces = [
            code_ref[source_ref[t], pl.ds(start, pair), :].astype(jnp.int32).astype(jnp.float32)
            for t in range(places)
        ]
        for half in range(2):
            stacked = jnp.concatenate(
                [
                    piece[half * block_size : (half + 1) * block_size] * scale_ref[t]
                    for t, piece in enumerate(pieces)
                ],
                axis=0,
            )
            turned = stacked.T
            for h in range(folds):
                out_ref[h * strip + r + half] = turned[h * width : (h + 1) * width]


def blocks_to_native(incoming, arrive_from, previous, width, levels, from_level, block_size):
    _, coded, _ = incoming.shape
    places = arrive_from.shape[0]
    folds = max(1, LANES // width)
    tail_at = coded - block_size
    height = 8 * folds
    first = from_level // height
    return pl.pallas_call(
        functools.partial(native_kernel, places=places, block_size=block_size, tail_at=tail_at),
        grid_spec=pltpu.PrefetchScalarGridSpec(
            num_scalar_prefetch=1,
            grid=(tail_at // block_size // 8,),
            in_specs=[pl.BlockSpec(memory_space=pltpu.VMEM)]
            + [pl.BlockSpec(memory_space=pl.ANY)] * len(previous),
            out_specs=pl.BlockSpec(
                (height, width, places * block_size), lambda g, a: (first + g, 0, 0)
            ),
            scratch_shapes=[pltpu.VMEM((places, block_size, LANES), jnp.float32)],
        ),
        out_shape=jax.ShapeDtypeStruct((levels, width, places * block_size), jnp.float32),
        input_output_aliases={2: 0} if previous else {},
        name="native",
    )(arrive_from, incoming, *previous)


def analysis_shards(
    background, obs_ensemble, obs_value, obs_weight, stencil, stencil_weight, block_target
):
    members = obs_ensemble.shape[3] * lax.axis_size("member")
    fill = LANES // math.gcd(background.shape[2], LANES)
    coded = coded_transforms(obs_ensemble[:, 0], obs_value[0, 0], obs_weight[0, 0], fill)
    points = coded.shape[0]
    member_count = lax.axis_size("member")
    band_index = lax.axis_index("member")
    levels, columns = background.shape[2], background.shape[4]
    group = math.gcd(levels, LANES)
    groups = levels // group
    cut = max(1, groups // 3)
    order = (band_index + jnp.arange(member_count, dtype=jnp.int32)) % member_count
    early, late = pack_lanes(background[:, 0].transpose(0, 2, 3, 1), order, cut)
    early = lax.all_to_all(early, "member", split_axis=0, concat_axis=0, tiled=True)
    late, block_target, stencil, stencil_weight, coded = lax.optimization_barrier(
        (late, block_target, stencil, stencil_weight, coded)
    )
    late = [late[step] for step in range(member_count)]
    left, right = halo_pair(coded, "region")
    left, *late = lax.optimization_barrier((left, *late))
    trio = jnp.concatenate([left, coded, right], axis=0)
    low, high = halo_pair(trio, "member")
    late_pieces = [late[0].reshape(-1, columns, LANES)]
    for step in range(1, member_count):
        ring = [(i, (i + step) % member_count) for i in range(member_count)]
        arrived = lax.ppermute(late[step], "member", ring)
        late_pieces.append(arrived.reshape(-1, columns, LANES))
    late_source = (band_index - jnp.arange(member_count, dtype=jnp.int32)) % member_count
    early_source = jnp.zeros((1,), jnp.int32)
    patch_index = lax.axis_index("region")
    patch_list = lax.axis_size("region")
    shard_width = members // member_count
    stencil_rows = stencil[0, 0]
    near_band = stencil_rows // (patch_list * points)
    near_patch = stencil_rows // points % patch_list
    local_index = (
        (near_band - band_index + 1) * 3 + (near_patch - patch_index + 1)
    ) * points + stencil_rows % points
    share = stencil_weight[0, 0] / jnp.sum(stencil_weight[0, 0], axis=0, keepdims=True)
    band_count = block_target.shape[0]
    per_device = block_target.shape[2]
    per_owner = band_count * per_device
    block_size = columns // per_device
    owners = block_target // per_owner
    places = block_target % per_owner
    patch_ids = jnp.arange(patch_list, dtype=jnp.int32)
    place_ids = jnp.arange(per_owner, dtype=jnp.int32)
    band_owners = lax.dynamic_index_in_dim(owners, band_index, 0, keepdims=False)
    my_owners = lax.dynamic_index_in_dim(band_owners, patch_index, 0, keepdims=False)
    block_ids = jnp.arange(per_device, dtype=jnp.int32)
    send_hit = my_owners[None, :] == patch_ids[:, None]
    send_from = jnp.sum(send_hit.astype(jnp.int32) * block_ids[None, :], axis=1)
    band_ids = jnp.arange(band_count, dtype=jnp.int32)
    source = band_ids[:, None, None] * patch_list + patch_ids[None, :, None] + 0 * places
    arrive_hit = (owners == patch_index)[None] & (places[None] == place_ids[:, None, None, None])
    arrive_from = jnp.sum(arrive_hit.astype(jnp.int32) * source[None], axis=(1, 2, 3))
    native = ()
    chunks = (
        (0, cut, [early.reshape(-1, columns, LANES)], early_source),
        (cut, groups, late_pieces, late_source),
    )
    for start, end, states, state_source in chunks:
        outgoing = columns_to_blocks(
            states, state_source, (low, trio, high), local_index, share, send_from, group,
            (end - start) * group, member_count, block_size,
        )
        outgoing = outgoing.reshape(member_count * patch_list, *outgoing.shape[2:])
        incoming = lax.all_to_all(
            outgoing, ("member", "region"), split_axis=0, concat_axis=0, tiled=True
        )
        native = (
            blocks_to_native(
                incoming, arrive_from, native, shard_width, levels, start * group, block_size
            ),
        )
    return native[0].reshape(1, levels, shard_width, per_owner * block_size)


def solution(mesh):
    in_specs = (
        P(None, "region", None, "member", None),
        P(None, "region", None, "member", None),
        P("member", "region", None, None),
        P("member", "region", None, None),
        P("member", "region", None, None),
        P("member", "region", None, None),
        P(),
    )
    out_specs = P("region", None, "member", None)
    return jax.shard_map(analysis_shards, mesh=mesh, in_specs=in_specs, out_specs=out_specs, check_vma=False)
```
